8 devices in a mesh: dp: 4 (over z, y, x), cp: 2 (over core).
Axes of the slice: x: 2, y: 2, z: 1, core: 2. Of those that a mesh axis runs over, the one named last changes fastest.
Arguments:
- x_in: bfloat16 [24, 1024, 1280], P('dp', 'cp')
- d_out: bfloat16 [24, 1024, 1280], P('dp', 'cp')
- w_q: bfloat16 [1280, 20, 64], replicated
- w_k: bfloat16 [1280, 20, 64], replicated
- w_v: bfloat16 [1280, 20, 64], replicated
- w_o: bfloat16 [20, 64, 1280], replicated
- w_up: bfloat16 [1280, 5120], replicated
- w_down: bfloat16 [5120, 1280], replicated
Outputs:
- output 1: bfloat16 [24, 1024, 1280], P('dp', 'cp')
- output 2: float32 [1280, 20, 64], replicated
- output 3: float32 [1280, 20, 64], replicated
- output 4: float32 [1280, 20, 64], replicated
- output 5: float32 [20, 64, 1280], replicated
- output 6: float32 [1280, 5120], replicated
- output 7: float32 [5120, 1280], replicated
All inputs are finite; a program needn't handle non-finite values.
Results may differ from the reference program's by a relative error of at most 0.018143.
Values are sent between devices in bfloat16 or wider.
A program may use at most 1 GiB of HBM per device.

```python
import jax
import jax.numpy as jnp
from jax import lax

BATCH_SIZE = 24
SEQ_LEN = 1024
D_MODEL = 1280
N_HEADS = 20
HEAD_DIM = 64
FFN_DIM = 5120
N_SHARDS = 8
Q_BLOCK = 256


def setup_inputs(seed: int = 0) -> dict:
    key_list = jax.random.split(jax.random.key(seed), 8)
    attn_width = N_HEADS * HEAD_DIM
    act_shape = (BATCH_SIZE, SEQ_LEN, D_MODEL)

    def draw_normal(key_part, arr_shape, std_dev):
        return (jax.random.normal(key_part, arr_shape, jnp.float32) * std_dev).astype(jnp.bfloat16)

    return {
        'x_in': draw_normal(key_list[0], act_shape, 1.0),
        'd_out': draw_normal(key_list[1], act_shape, 1.0),
        'w_q': draw_normal(key_list[2], (D_MODEL, N_HEADS, HEAD_DIM), D_MODEL ** -0.5),
        'w_k': draw_normal(key_list[3], (D_MODEL, N_HEADS, HEAD_DIM), D_MODEL ** -0.5),
        'w_v': draw_normal(key_list[4], (D_MODEL, N_HEADS, HEAD_DIM), D_MODEL ** -0.5),
        'w_o': draw_normal(key_list[5], (N_HEADS, HEAD_DIM, D_MODEL), attn_width ** -0.5),
        'w_up': draw_normal(key_list[6], (D_MODEL, FFN_DIM), D_MODEL ** -0.5),
        'w_down': draw_normal(key_list[7], (FFN_DIM, D_MODEL), FFN_DIM ** -0.5),
    }


def keep_bf16(values):
    return values.astype(jnp.bfloat16).astype(jnp.float32)


def stored_positions():
    n_blocks = SEQ_LEN // Q_BLOCK
    stored = jnp.arange(n_blocks)
    owner_rank = stored // 2
    seq_block = owner_rank + (stored % 2) * (n_blocks - 1 - 2 * owner_rank)
    return (seq_block[:, None] * Q_BLOCK + jnp.arange(Q_BLOCK)[None, :]).reshape(SEQ_LEN)


def attend_block(q_rows, pos_rows, key_seq, val_seq, positions):
    scores = jnp.einsum('qhe,khe->hqk', q_rows, key_seq) * (HEAD_DIM ** -0.5)
    scores = jnp.where(positions[None, None, :] <= pos_rows[None, :, None], scores, -1e30)
    prob_b = keep_bf16(jax.nn.softmax(scores, axis=-1))
    return keep_bf16(jnp.einsum('hqk,khe->qhe', prob_b, val_seq))


def attend_sequence(q_seq, key_seq, val_seq, positions):
    n_blocks = SEQ_LEN // Q_BLOCK
    q_blocks = q_seq.reshape(n_blocks, Q_BLOCK, N_HEADS, HEAD_DIM)
    pos_blocks = positions.reshape(n_blocks, Q_BLOCK)
    block_fn = jax.checkpoint(attend_block)
    outs = lax.map(lambda block_pair: block_fn(block_pair[0], block_pair[1], key_seq, val_seq, positions), (q_blocks, pos_blocks))
    return outs.reshape(SEQ_LEN, N_HEADS, HEAD_DIM)


def reference(x_in, d_out, w_q, w_k, w_v, w_o, w_up, w_down):
    positions = stored_positions()

    def forward(x_f32, wq_f32, wk_f32, wv_f32, wo_f32, wu_f32, wd_f32):
        q_seq = keep_bf16(jnp.einsum('bsd,dhe->bshe', x_f32, wq_f32))
        k_seq = keep_bf16(jnp.einsum('bsd,dhe->bshe', x_f32, wk_f32))
        v_seq = keep_bf16(jnp.einsum('bsd,dhe->bshe', x_f32, wv_f32))
        attn_out = lax.map(lambda qkv_rows: attend_sequence(qkv_rows[0], qkv_rows[1], qkv_rows[2], positions), (q_seq, k_seq, v_seq))
        hidden = keep_bf16(x_f32 + jnp.einsum('bshe,hed->bsd', attn_out, wo_f32))
        up_pre = keep_bf16(jnp.einsum('bsd,df->bsf', hidden, wu_f32))
        act_val = keep_bf16(jax.nn.gelu(up_pre, approximate=True))
        return (hidden + jnp.einsum('bsf,fd->bsd', act_val, wd_f32)).astype(jnp.bfloat16)

    out_val, pullback = jax.vjp(
        forward,
        x_in.astype(jnp.float32),
        w_q.astype(jnp.float32),
        w_k.astype(jnp.float32),
        w_v.astype(jnp.float32),
        w_o.astype(jnp.float32),
        w_up.astype(jnp.float32),
        w_down.astype(jnp.float32),
    )
    grads = pullback(d_out)
    return (
        grads[0].astype(jnp.bfloat16),
        grads[1] / N_SHARDS,
        grads[2] / N_SHARDS,
        grads[3] / N_SHARDS,
        grads[4] / N_SHARDS,
        grads[5] / N_SHARDS,
        grads[6] / N_SHARDS,
    )
```

```python
import functools
import jax
import jax.numpy as jnp
from jax import lax
from jax.experimental import pallas as pl
from jax.experimental.pallas import tpu as pltpu
from jax.sharding import PartitionSpec as P

NEG_BIG = -1e30
BLK = 256
PAIR = 128
HEAD = 64
PLACE = ((0, 0), (1, 0), (1, BLK), (0, BLK))
COL_OFF = (0, 4 * BLK, 7 * BLK, 9 * BLK)
P_ROWS = 10 * BLK
SCALE = 0.125


def dot(a, b, dims):
    return lax.dot_general(a, b, (dims, ((), ())), preferred_element_type=jnp.float32)


def rows_of(ref, blk):
    part, off = PLACE[blk]
    return ref[part, 0, off:off + BLK, :]


def head_mask(head, value):
    lane = lax.broadcasted_iota(jnp.int32, (1, PAIR), 1)
    inside = (lane >= head * HEAD) & (lane < (head + 1) * HEAD)
    return jnp.where(inside, jnp.float32(value), jnp.float32(0.0)).astype(jnp.bfloat16)


def attn_fwd_kernel(q_ref, k_ref, v_ref, o_ref, p_ref, s_scr, vt_scr, ot_scr):
    for b in range(4):
        vt_scr[:, b * BLK:(b + 1) * BLK] = rows_of(v_ref, b).T
    row_i = lax.broadcasted_iota(jnp.int32, (BLK, BLK), 0)
    col_i = lax.broadcasted_iota(jnp.int32, (BLK, BLK), 1)
    keep = row_i >= col_i
    for i in range(4):
        width = (i + 1) * BLK
        for head in range(2):
            buf = (2 * i + head) % 2
            q_m = rows_of(q_ref, i) * head_mask(head, SCALE)
            for kb in range(i + 1):
                s = dot(q_m, rows_of(k_ref, kb), ((1,), (1,)))
                if kb == i:
                    s = jnp.where(keep, s, NEG_BIG)
                s_scr[buf, :, kb * BLK:(kb + 1) * BLK] = s
            step = 32
            for r in range(0, BLK, step):
                s = s_scr[buf, r:r + step, 0:width]
                e = jnp.exp(s - jnp.max(s, axis=1, keepdims=True))
                p = (e * (1.0 / jnp.sum(e, axis=1, keepdims=True))).astype(jnp.bfloat16)
                for kb in range(i + 1):
                    at = COL_OFF[kb] + (i - kb) * BLK + r
                    p_ref[0, 0, head, at:at + step, :] = p[:, kb * BLK:(kb + 1) * BLK]
            acc = None
            for kb in range(i + 1):
                at = COL_OFF[kb] + (i - kb) * BLK
                part = dot(vt_scr[head * HEAD:(head + 1) * HEAD, kb * BLK:(kb + 1) * BLK],
                           p_ref[0, 0, head, at:at + BLK, :], ((1,), (1,)))
                acc = part if acc is None else acc + part
            ot_scr[head * HEAD:(head + 1) * HEAD, :] = acc
        part, off = PLACE[i]
        o_ref[part, 0, off:off + BLK, :] = ot_scr[...].T.astype(jnp.bfloat16)


def attn_bwd_kernel(q_ref, k_ref, v_ref, g_ref, o_ref, p_ref, dq_ref, dk_ref, dv_ref,
                    qt_scr, kt_scr, gt_scr, ds_scr, dq_scr, dk_scr, dv_scr):
    for b in range(4):
        cols = slice(b * BLK, (b + 1) * BLK)
        qt_scr[:, cols] = (rows_of(q_ref, b) * jnp.bfloat16(SCALE)).T
        kt_scr[:, cols] = rows_of(k_ref, b).T
        gt_scr[:, cols] = rows_of(g_ref, b).T
    lane = lax.broadcasted_iota(jnp.int32, (BLK, PAIR), 1)
    for head in range(2):
        hs = slice(head * HEAD, (head + 1) * HEAD)
        inside = (lane >= head * HEAD) & (lane < (head + 1) * HEAD)
        for i in range(4):
            g_i = rows_of(g_ref, i)
            prod = g_i.astype(jnp.float32) * rows_of(o_ref, i).astype(jnp.float32)
            delta = jnp.sum(jnp.where(inside, prod, 0.0), axis=1, keepdims=True)
            g_m = g_i * head_mask(head, 1.0)
            acc = None
            for kb in range(i + 1):
                at = COL_OFF[kb] + (i - kb) * BLK
                dp = dot(g_m, rows_of(v_ref, kb), ((1,), (1,))).astype(jnp.bfloat16).astype(jnp.float32)
                p = p_ref[0, 0, head, at:at + BLK, :].astype(jnp.float32)
                ds = (p * (dp - delta)).astype(jnp.bfloat16)
                ds_scr[head, at:at + BLK, :] = ds
                part = dot(kt_scr[hs, kb * BLK:(kb + 1) * BLK], ds, ((1,), (1,)))
                acc = part if acc is None else acc + part
            dq_scr[hs, i * BLK:(i + 1) * BLK] = acc
        for kb in range(4):
            at, n = COL_OFF[kb], (4 - kb) * BLK
            dk_scr[hs, kb * BLK:(kb + 1) * BLK] = dot(qt_scr[hs, kb * BLK:4 * BLK], ds_scr[head, at:at + n, :], ((1,), (0,)))
            dv_scr[hs, kb * BLK:(kb + 1) * BLK] = dot(gt_scr[hs, kb * BLK:4 * BLK], p_ref[0, 0, head, at:at + n, :], ((1,), (0,)))
    for b in range(4):
        part, off = PLACE[b]
        cols = slice(b * BLK, (b + 1) * BLK)
        dq_ref[part, 0, off:off + BLK, :] = (dq_scr[:, cols] * SCALE).T.astype(jnp.bfloat16)
        dk_ref[part, 0, off:off + BLK, :] = dk_scr[:, cols].T.astype(jnp.bfloat16)
        dv_ref[part, 0, off:off + BLK, :] = dv_scr[:, cols].T.astype(jnp.bfloat16)


def attention_calls(n_seq, n_pair, half):
    act = pl.BlockSpec((2, 1, half, PAIR), lambda b, h: (0, b, 0, h))
    prob = pl.BlockSpec((1, 1, 2, P_ROWS, BLK), lambda b, h: (b, h, 0, 0, 0))
    act_shape = jax.ShapeDtypeStruct((2, n_seq, half, n_pair * PAIR), jnp.bfloat16)
    prob_shape = jax.ShapeDtypeStruct((n_seq, n_pair, 2, P_ROWS, BLK), jnp.bfloat16)
    seq = 2 * half
    blocks = n_seq * n_pair * 2 * 10
    params = pltpu.CompilerParams(dimension_semantics=('arbitrary', 'arbitrary'), vmem_limit_bytes=48 * 2 ** 20)
    fwd = pl.pallas_call(
        attn_fwd_kernel, grid=(n_seq, n_pair), name='attn_fwd',
        in_specs=[act, act, act], out_specs=[act, prob], out_shape=[act_shape, prob_shape],
        scratch_shapes=[pltpu.VMEM((2, BLK, seq), jnp.float32), pltpu.VMEM((PAIR, seq), jnp.bfloat16),
                        pltpu.VMEM((PAIR, BLK), jnp.float32)],
        compiler_params=params,
        cost_estimate=pl.CostEstimate(flops=blocks * 4 * BLK * BLK * 256, bytes_accessed=blocks * BLK * BLK * 2,
                                      transcendentals=blocks * BLK * BLK))
    bwd = pl.pallas_call(
        attn_bwd_kernel, grid=(n_seq, n_pair), name='attn_bwd',
        in_specs=[act] * 5 + [prob], out_specs=[act] * 3, out_shape=[act_shape] * 3,
        scratch_shapes=[pltpu.VMEM((PAIR, seq), jnp.bfloat16)] * 3
        + [pltpu.VMEM((2, P_ROWS, BLK), jnp.bfloat16)] + [pltpu.VMEM((PAIR, seq), jnp.float32)] * 3,
        compiler_params=params,
        cost_estimate=pl.CostEstimate(flops=blocks * 8 * BLK * BLK * 256, bytes_accessed=blocks * BLK * BLK * 2,
                                      transcendentals=0))
    return fwd, bwd


def gelu(u):
    return jax.nn.gelu(u, approximate=True)


def solution(mesh):
    n_total = mesh.shape['dp'] * mesh.shape['cp']
    inv = 1.0 / n_total
    swap = [(0, 1), (1, 0)]
    f32, bf16 = jnp.float32, jnp.bfloat16

    def partner(tree):
        return lax.ppermute(tree, 'cp', swap)

    def across(item, bit):
        return lax.ppermute(item, 'dp', [(i, i ^ bit) for i in range(4)])

    def chip_sum(item):
        dp = lax.axis_index('dp')
        out = []
        n = item.shape[0] // 2
        for color, (bit_a, bit_b) in enumerate(((1, 2), (2, 1))):
            at_a = (dp // bit_a) % 2
            at_b = (dp // bit_b) % 2
            start = color * n

            def rows(arr, which, size, base=0):
                return lax.dynamic_slice_in_dim(arr, base + which * size, size, 0)

            got = across(rows(item, 1 - at_a, n // 2, start), bit_a)
            half = rows(item, at_a, n // 2, start) + got
            got = across(rows(half, 1 - at_b, n // 4), bit_b)
            mine = rows(half, at_b, n // 4) + got
            got = across(mine, bit_b)
            both = lax.dynamic_slice_in_dim(jnp.concatenate([mine, got, mine], axis=0), at_b * (n // 4), n // 2, 0)
            far = across(both, bit_a)
            out.append((start + at_a * (n // 2), both))
            out.append((start + (1 - at_a) * (n // 2), far))
        return out

    def per_device(x_in, d_out, w_q, w_k, w_v, w_o, w_up, w_down):
        rank = lax.axis_index('cp')
        b_loc, half, d_model = x_in.shape
        n_heads, head_dim = w_q.shape[1], w_q.shape[2]
        width = n_heads * head_dim
        f_dim = w_up.shape[1]
        n_seq = b_loc // 2
        tokens = b_loc * half
        attn_fwd, attn_bwd = attention_calls(n_seq, width // PAIR, half)

        def reshard(item):
            return lax.all_to_all(item, 'cp', 0, 0, tiled=True)

        def to_pairs(item):
            return item.reshape(2, n_seq, half, width)

        def flat(item):
            return item.reshape(tokens, -1)

        x_t = flat(reshard(x_in))
        g_t = flat(reshard(d_out))
        wq_t = jnp.transpose(w_q, (1, 2, 0)).reshape(width, d_model)
        wk_t = jnp.transpose(w_k, (1, 2, 0)).reshape(width, d_model)
        wv_t = jnp.transpose(w_v, (1, 2, 0)).reshape(width, d_model)
        wo = w_o.reshape(width, d_model)
        q = dot(x_t, wq_t, ((1,), (1,))).astype(bf16)
        k = dot(x_t, wk_t, ((1,), (1,))).astype(bf16)
        v = dot(x_t, wv_t, ((1,), (1,))).astype(bf16)
        o, prob = attn_fwd(to_pairs(q), to_pairs(k), to_pairs(v))
        o_t = flat(o)
        hidden = (x_t.astype(f32) + dot(o_t, wo, ((1,), (0,)))).astype(bf16)

        def pick(item, which, off, size, axis):
            n_half = item.shape[axis] // 2
            return lax.dynamic_slice_in_dim(item, which * n_half + off, size, axis)

        other = 1 - rank

        class Gather:
            def __init__(self, shape, axis):
                self.out = jnp.zeros(shape, f32)
                self.axis = axis
                self.n_half = shape[axis] // 2

            def put(self, item, row, col):
                self.out = lax.dynamic_update_slice(self.out, item, (row, col))

            def add(self, off, mine, theirs, name):
                for at, item in chip_sum(mine + partner(theirs)):
                    back = partner(item)
                    for which, block in ((rank, item), (other, back)):
                        base = which * self.n_half + off
                        if self.axis == 0:
                            self.put(block, base + at, 0)
                        else:
                            self.put(block, at, base)

        n_sub = 2
        sub = f_dim // 2 // n_sub
        down, up = Gather(w_down.shape, 0), Gather(w_up.shape, 1)
        pre = {}
        for c in range(n_sub):
            parts = []
            for which, key in ((other, 'o'), (rank, 'm')):
                u = dot(hidden, pick(w_up, which, c * sub, sub, 1), ((1,), (0,))).astype(bf16)
                pre[key, c] = u
                act = gelu(u.astype(f32)).astype(bf16)
                parts.append(dot(act, g_t, ((0,), (0,))) * inv)
            down.add(c * sub, parts[1], parts[0], f'down{c}')
        g_hid = g_t.astype(f32)
        g_pre = {}
        for c in range(n_sub):
            parts = []
            for which, key in ((other, 'o'), (rank, 'm')):
                g_act = dot(g_t, pick(w_down, which, c * sub, sub, 0), ((1,), (1,))).astype(bf16)
                _, pull = jax.vjp(gelu, pre[key, c].astype(f32))
                gp = pull(g_act.astype(f32))[0].astype(bf16)
                g_pre[key, c] = gp
                parts.append(dot(hidden, gp, ((0,), (0,))) * inv)
            up.add(c * sub, parts[1], parts[0], f'up{c}')
        gp_all = jnp.concatenate([g_pre[key, c] for key in ('m', 'o') for c in range(n_sub)], axis=1)
        w_up_all = jnp.concatenate([pick(w_up, which, 0, f_dim // 2, 1) for which in (rank, other)], axis=1)
        g_hid = (g_hid + dot(gp_all, w_up_all, ((1,), (1,)))).astype(bf16)
        g_attn = dot(g_hid, wo, ((1,), (1,))).astype(bf16)
        hw = width // 2
        g_o = Gather((width, d_model), 0)
        parts = [dot(pick(o_t, which, 0, hw, 1), g_hid, ((0,), (0,))) * inv for which in (other, rank)]
        g_o.add(0, parts[1], parts[0], 'o')
        dq, dk, dv = attn_bwd(to_pairs(q), to_pairs(k), to_pairs(v), to_pairs(g_attn), to_pairs(o_t), prob)
        dq, dk, dv = flat(dq), flat(dk), flat(dv)
        outs = []
        for name, item in (('v', dv), ('k', dk), ('q', dq)):
            acc = Gather((width, d_model), 0)
            parts = [dot(pick(item, which, 0, hw, 1), x_t, ((0,), (0,))) * inv for which in (other, rank)]
            acc.add(0, parts[1], parts[0], name)
            outs.append(jnp.transpose(acc.out.reshape(n_heads, head_dim, d_model), (2, 0, 1)))
        g_v, g_k, g_q = outs
        d_x = (g_hid.astype(f32) + dot(dq, wq_t, ((1,), (0,))) + dot(dk, wk_t, ((1,), (0,)))
               + dot(dv, wv_t, ((1,), (0,)))).astype(bf16)
        d_x = reshard(d_x.reshape(b_loc, half, d_model))
        return d_x, g_q, g_k, g_v, g_o.out.reshape(w_o.shape), up.out, down.out

    act_spec = P('dp', 'cp', None)
    return jax.shard_map(per_device, mesh=mesh,
                         in_specs=(act_spec, act_spec, P(), P(), P(), P(), P(), P()),
                         out_specs=(act_spec, P(), P(), P(), P(), P(), P()),
                         check_vma=False)
```
